512 devices in a mesh: grp: 2 (over y), seq: 32 (over z, core), head: 8 (over x).
Axes of the slice: x: 8, y: 2, z: 16, core: 2. Of those that a mesh axis runs over, the one named last changes fastest.
The devices are a block of a 8x8x16 slice.
Arguments:
- draft_features: bfloat16 [16384, 8192], P(('grp', 'seq'), 'head'), parts along dimension 0, may hold values from -6 to 6
- w_key: bfloat16 [8192, 1024], P(None, 'head'), may hold values from -0.0625 to 0.0625
- w_value: bfloat16 [8192, 1024], P(None, 'head'), may hold values from -0.0625 to 0.0625
- accepted: int32 [2048], P(('grp', 'seq')), parts along dimension 0, may hold values from 1 to 8
- owner_group: int32 [2048], P(('grp', 'seq')), parts along dimension 0, may hold values from 0 to 31, as said below
- page_slot: int32 [2048], P(('grp', 'seq')), parts along dimension 0, may hold values from 0 to 63, as said below
Outputs:
- key_cache: bfloat16 [4096, 8, 1024], P(('grp', 'seq'), None, 'head'), parts along dimension 0
- value_cache: bfloat16 [4096, 8, 1024], P(('grp', 'seq'), None, 'head'), parts along dimension 0
The draws below stay inside these ranges and needn't reach their ends.
There are 2 independent parts, one for each index of `grp`. The reference program is written for one: setup_inputs(seed, part) draws one part's arguments, and reference() takes and returns one part's arrays. A program takes and returns all parts, laid end to end along the dimension named above; an argument that names none is the same for every part. Nothing has to cross between parts.
Inputs may be any that keep to these rules, and one draw needn't show every extreme that they name: `owner_group`: the requests of one index of seq go to exactly 16 distinct owners, 2 to each; some owner receives 64 requests. `page_slot`: the requests of one owner have distinct slots.
All inputs are finite; a program needn't handle non-finite values.
Results may differ from the reference program's by a relative error of at most 0.001.
Values may be sent and summed in bfloat16 or wider, within the bound.
No kernel may reach another device: no remote copies, remote signals or barrier semaphores. Data moves between devices by JAX's collectives and lax.ppermute only.
A program may use at most 64 MiB of HBM per device.

```python
import jax
import jax.numpy as jnp

D = 8192
KVH = 8
HD = 128
DRAFT = 8
REQ_DEV = 32
CAP = 2
SLOT_DEV = 64
REQUESTS = 1024
ROWS = 8192
N_SEQ = 32


def route_table(key):
    picks = REQ_DEV // CAP
    base = jax.random.fold_in(key, 7)
    key_star, key_scores, key_order, key_pages = jax.random.split(base, 4)
    star = jax.random.randint(key_star, (), 0, N_SEQ)
    scores = jax.vmap(lambda sub: jax.random.permutation(sub, N_SEQ))(jax.random.split(key_scores, N_SEQ))
    scores = jnp.where(jnp.arange(N_SEQ)[None, :] == star, -1, scores)
    ranked = jnp.argsort(scores, axis=1, stable=True).astype(jnp.int32)
    chosen = ranked[:, :picks]
    shuffled = jax.vmap(lambda sub: jax.random.permutation(sub, REQ_DEV))(jax.random.split(key_order, N_SEQ))
    owners = jnp.take_along_axis(chosen, (shuffled // CAP).astype(jnp.int32), axis=1).reshape(-1).astype(jnp.int32)
    priority = jax.random.permutation(key_pages, N_SEQ * REQ_DEV)
    same_owner = owners[:, None] == owners[None, :]
    earlier = priority[None, :] < priority[:, None]
    pages = jnp.sum(jnp.where(same_owner & earlier, 1, 0), axis=1).astype(jnp.int32)
    return (owners, pages)


def draw_owner_group(key, part):
    return route_table(key)[0]


def draw_page_slot(key, part):
    return route_table(key)[1]


def plant(values, rng, low, top_value):
    longest = values.shape.index(max(values.shape))
    spots = []
    for shift in (0, 1):
        where = [jax.random.randint(jax.random.fold_in(rng, axis), (), 0, length) for axis, length in enumerate(values.shape)]
        where[longest] = (where[longest] + shift) % values.shape[longest]
        spots.append(tuple(where))
    return values.at[spots[0]].set(low).at[spots[1]].set(top_value)


def shard_levels(stream_key, extent, pieces, low, high):
    def one(position, parts):
        draws = jax.random.uniform(jax.random.fold_in(jax.random.fold_in(stream_key, 6), position), (parts,), jnp.float32, low / len(pieces), high / len(pieces))
        return jnp.repeat(jnp.exp(draws), extent[position] // parts).reshape((-1,) + (1,) * (len(extent) - position - 1))

    gain = one(*pieces[0])
    for cut in pieces[1:]:
        gain = gain * one(*cut)
    return gain


def noise(stream_key, dims, scale, most, cuts=(), held_as=jnp.bfloat16):
    array = jax.random.normal(stream_key, dims, jnp.float32) * scale
    if len(cuts) > 0:
        array = shard_levels(stream_key, dims, cuts, -0.22, 0.18) * array
    return jnp.clip(array, min=-most, max=most).astype(held_as)


def setup_inputs(seed: int = 0, part: int = 0) -> dict:
    key_of = jax.random.split(jax.random.key(seed), 7)
    own_keys = jax.random.split(jax.random.fold_in(key_of[6], part), 7)
    return {
        "draft_features": noise(own_keys[0], (ROWS, D), 1.0, 6.0, ((0, 32), (1, 8))),
        "w_key": noise(key_of[1], (D, KVH * HD), D ** -0.5, 0.0625, ((1, 8),)),
        "w_value": noise(key_of[2], (D, KVH * HD), D ** -0.5, 0.0625, ((1, 8),)),
        "accepted": plant(jax.random.randint(own_keys[3], (REQUESTS,), 1, DRAFT + 1), jax.random.fold_in(own_keys[3], 1), 1, DRAFT).astype(jnp.int32),
        "owner_group": draw_owner_group(jax.random.fold_in(jax.random.fold_in(key_of[6], part), 71), part),
        "page_slot": draw_page_slot(jax.random.fold_in(jax.random.fold_in(key_of[6], part), 71), part),
    }


def reference(draft_features, w_key, w_value, accepted, owner_group, page_slot):
    key_rows = jnp.dot(draft_features, w_key, preferred_element_type=jnp.float32).astype(jnp.bfloat16)
    value_rows = jnp.dot(draft_features, w_value, preferred_element_type=jnp.float32).astype(jnp.bfloat16)
    live_rows = jnp.arange(DRAFT, dtype=jnp.int32)[None, :] < accepted[:, None]
    key_rows = jnp.where(live_rows[:, :, None], key_rows.reshape(REQUESTS, DRAFT, KVH * HD), jnp.zeros((), key_rows.dtype))
    value_rows = jnp.where(live_rows[:, :, None], value_rows.reshape(REQUESTS, DRAFT, KVH * HD), jnp.zeros((), value_rows.dtype))
    slot_ids = (owner_group * SLOT_DEV + page_slot).astype(jnp.int32)
    key_cache = jnp.zeros((N_SEQ * SLOT_DEV, DRAFT, KVH * HD), key_rows.dtype).at[slot_ids].set(key_rows)
    value_cache = jnp.zeros((N_SEQ * SLOT_DEV, DRAFT, KVH * HD), value_rows.dtype).at[slot_ids].set(value_rows)
    return key_cache, value_cache
```

```python
import functools

import jax
import jax.numpy as jnp
from jax import lax
from jax.experimental import pallas as pl
from jax.experimental.pallas import tpu as pltpu
from jax.sharding import PartitionSpec as P

CHUNKS = 2


def gather_ring(block):
    heads = lax.axis_size("head")
    up = [(i, (i + 1) % heads) for i in range(heads)]
    down = [(i, (i - 1) % heads) for i in range(heads)]
    own = jnp.split(block, CHUNKS, axis=0)
    held = [(0, own)]
    rising, falling = list(own), list(own)
    for step in range(1, (heads + 1) // 2):
        for c in range(CHUNKS):
            rising[c] = lax.ppermute(rising[c], "head", up)
            falling[c] = lax.ppermute(falling[c], "head", down)
        held.append((heads - step, list(rising)))
        held.append((step, list(falling)))
    if heads % 2 == 0:
        last = [
            lax.ppermute(rising[c], "head", up) if c % 2 == 0 else lax.ppermute(falling[c], "head", down)
            for c in range(CHUNKS)
        ]
        held.append((heads // 2, last))
    return held


def iota(shape, dim):
    return lax.broadcasted_iota(jnp.int32, shape, dim)


def project_pack_kernel(offsets, slot_cap, draft, me_ref, route_ref, *refs):
    blocks = refs[: len(offsets) * CHUNKS]
    wk_ref, wv_ref, out_ref = refs[len(offsets) * CHUNKS :]
    depth = blocks[0].shape[1]
    heads = len(offsets)
    total = None
    for i, offset in enumerate(offsets):
        rows = jnp.concatenate([b[...] for b in blocks[i * CHUNKS : (i + 1) * CHUNKS]], axis=0)
        origin = lax.rem(me_ref[0] + offset, heads)
        at = pl.ds(pl.multiple_of(origin * depth, depth), depth)
        weights = jnp.concatenate([wk_ref[at, :], wv_ref[at, :]], axis=1)
        part = jnp.dot(rows, weights, preferred_element_type=jnp.float32)
        total = part if total is None else total + part
    projected = total.astype(jnp.bfloat16)
    req = route_ref.shape[1]
    accepted = route_ref[0:1, :].astype(jnp.float32)
    owner = route_ref[1:2, :].astype(jnp.float32)
    page = route_ref[2:3, :].astype(jnp.float32)
    diagonal = iota((req, req), 0) == iota((req, req), 1)
    owner_col = jnp.sum(jnp.where(diagonal, owner, 0.0), axis=1, keepdims=True)
    earlier = (owner_col == owner) & (iota((req, req), 0) < iota((req, req), 1))
    within = jnp.sum(jnp.where(earlier, 1.0, 0.0), axis=0, keepdims=True)
    slot = owner * slot_cap + within
    row_count = req * draft
    lane, sub = iota((req, row_count), 1), iota((req, row_count), 0)
    mine = (lane >= sub * draft) & (lane < sub * draft + draft)
    slot_col = jnp.sum(jnp.where(diagonal, slot, 0.0), axis=1, keepdims=True)
    accepted_col = jnp.sum(jnp.where(diagonal, accepted, 0.0), axis=1, keepdims=True)
    draft_row = (lane - sub * draft).astype(jnp.float32)
    wanted = jnp.where(
        mine & (draft_row < accepted_col), slot_col * draft + draft_row + 1.0, 0.0
    )
    target = jnp.sum(wanted, axis=0, keepdims=True) - 1.0
    owners = out_ref.shape[0]
    slots = owners * slot_cap
    select = jnp.where(
        iota((slots * draft, row_count), 0).astype(jnp.float32) == target, 1.0, 0.0
    ).astype(jnp.bfloat16)
    packed = jnp.dot(select, projected, preferred_element_type=jnp.float32).astype(jnp.bfloat16)
    head_cols = wk_ref.shape[1]
    span = slot_cap * draft
    out_ref[:, 0:span, :] = packed[:, :head_cols].reshape(owners, span, head_cols)
    out_ref[:, span : 2 * span, :] = packed[:, head_cols:].reshape(owners, span, head_cols)
    part_lanes = head_cols // slot_cap
    dest = lax.div(iota((owners * draft, req), 0), draft).astype(jnp.float32)
    note_lane = iota((owners * draft, head_cols), 1)
    notes = jnp.full((owners * draft, head_cols), -1.0, jnp.float32)
    for s in range(slot_cap):
        found = jnp.sum(
            jnp.where(dest * slot_cap + s == slot, page + 1.0, 0.0), axis=1, keepdims=True
        ) - 1.0
        notes = jnp.where(note_lane >= s * part_lanes, found, notes)
    out_ref[:, 2 * span :, :] = notes.astype(jnp.bfloat16).reshape(owners, draft, head_cols)


def place_kernel(slot_cap, arrived_ref, key_ref, value_ref):
    sources, _, head_cols = arrived_ref.shape
    pages, draft, _ = key_ref.shape
    span = slot_cap * draft
    rows = sources * draft
    part_lanes = head_cols // slot_cap
    notes = arrived_ref[:, 2 * span :, :].reshape(rows, head_cols).astype(jnp.float32)
    draft_row = lax.rem(iota((rows, 1), 0), draft).astype(jnp.float32)
    spot = iota((rows, pages * draft), 1).astype(jnp.float32)
    total = None
    for s in range(slot_cap):
        page = notes[:, s * part_lanes : s * part_lanes + 1]
        goes = jnp.where(page >= 0.0, page * draft + draft_row, -1.0)
        select = jnp.where(goes == spot, 1.0, 0.0).astype(jnp.bfloat16)
        keys = arrived_ref[:, s * draft : (s + 1) * draft, :].reshape(rows, head_cols)
        values = arrived_ref[:, span + s * draft : span + (s + 1) * draft, :].reshape(rows, head_cols)
        both = jnp.concatenate([keys, values], axis=1)
        part = lax.dot_general(
            select, both, (((0,), (0,)), ((), ())), preferred_element_type=jnp.float32
        )
        total = part if total is None else total + part
    placed = total.astype(jnp.bfloat16)
    key_ref[...] = placed[:, :head_cols].reshape(pages, draft, head_cols)
    value_ref[...] = placed[:, head_cols:].reshape(pages, draft, head_cols)


def local(draft_features, w_key, w_value, accepted, owner_group, page_slot):
    req_dev = accepted.shape[0]
    draft = draft_features.shape[0] // req_dev
    depth = draft_features.shape[1]
    head_cols = w_key.shape[1]
    seq_count = lax.axis_size("seq")
    slot_cap = max(2, 2 * req_dev // seq_count)
    slot_total = slot_cap * seq_count
    route = jnp.stack([accepted, owner_group, page_slot])
    me = lax.axis_index("head").astype(jnp.int32).reshape(1)
    held = gather_ring(draft_features)
    offsets = tuple(offset for offset, _ in held)
    blocks = [b for _, chunks in held for b in chunks]
    vmem = pl.BlockSpec(memory_space=pltpu.VMEM)
    note_rows = 2 * slot_cap * draft + draft
    packed = pl.pallas_call(
        functools.partial(project_pack_kernel, offsets, slot_cap, draft),
        out_shape=jax.ShapeDtypeStruct((seq_count, note_rows, head_cols), jnp.bfloat16),
        in_specs=[pl.BlockSpec(memory_space=pltpu.SMEM), vmem] + [vmem] * (len(blocks) + 2),
        out_specs=vmem,
        cost_estimate=pl.CostEstimate(
            flops=4 * req_dev * draft * depth * len(offsets) * head_cols,
            bytes_accessed=2 * (req_dev * draft + 2 * head_cols) * depth * len(offsets),
            transcendentals=0,
        ),
        name="project_pack",
    )(me, route, *blocks, w_key, w_value)
    arrived = lax.all_to_all(packed, "seq", split_axis=0, concat_axis=0, tiled=True)
    cache = jax.ShapeDtypeStruct((slot_total, draft, head_cols), jnp.bfloat16)
    return pl.pallas_call(
        functools.partial(place_kernel, slot_cap),
        out_shape=(cache, cache),
        in_specs=[vmem],
        out_specs=(vmem, vmem),
        name="place",
    )(arrived)


def solution(mesh):
    placed = (
        P(("grp", "seq"), "head"),
        P(None, "head"),
        P(None, "head"),
        P(("grp", "seq")),
        P(("grp", "seq")),
        P(("grp", "seq")),
    )
    return jax.shard_map(
        local,
        mesh=mesh,
        in_specs=placed,
        out_specs=(P(("grp", "seq"), None, "head"), P(("grp", "seq"), None, "head")),
        check_vma=False,
    )
```

```python
import functools

import jax
import jax.numpy as jnp
from jax import lax
from jax.experimental import pallas as pl
from jax.experimental.pallas import tpu as pltpu
from jax.sharding import PartitionSpec as P

CHUNKS = 2
PROJECT_VMEM = 50 * 2**20
OTHER_VMEM = 12 * 2**20


def gather_ring(block):
    heads = lax.axis_size("head")
    up = [(i, (i + 1) % heads) for i in range(heads)]
    down = [(i, (i - 1) % heads) for i in range(heads)]
    own = jnp.split(block, CHUNKS, axis=0)
    held = [(0, own)]
    rising, falling = list(own), list(own)
    for step in range(1, (heads + 1) // 2):
        for c in range(CHUNKS):
            rising[c] = lax.ppermute(rising[c], "head", up)
            falling[c] = lax.ppermute(falling[c], "head", down)
        held.append((heads - step, list(rising)))
        held.append((step, list(falling)))
    if heads % 2 == 0:
        last = [
            lax.ppermute(rising[c], "head", up) if c % 2 == 0 else lax.ppermute(falling[c], "head", down)
            for c in range(CHUNKS)
        ]
        held.append((heads // 2, last))
    return held


def iota(shape, dim):
    return lax.broadcasted_iota(jnp.int32, shape, dim)


def project_kernel(offsets, slot_cap, draft, me_ref, accepted_ref, owner_ref, page_ref, wk_ref, wv_ref, *refs):
    count = len(offsets) - 1
    blocks = refs[: count * CHUNKS]
    total_ref, lastk_ref, lastv_ref, select_ref, notes_ref, weights, routes, sems = refs[count * CHUNKS :]
    depth, head_cols = blocks[0].shape[1], wk_ref.shape[1]
    heads = len(offsets)
    fetches = []
    for i, ref in enumerate((accepted_ref, owner_ref, page_ref)):
        fetches.append(pltpu.make_async_copy(ref, routes.at[i], sems.at[2 * heads + i]))
    for i, offset in enumerate(offsets):
        origin = lax.rem(me_ref[0] + offset, heads)
        at = pl.ds(pl.multiple_of(origin * depth, depth), depth)
        to = (weights.at[i, 0], weights.at[i, 1]) if i < count else (lastk_ref, lastv_ref)
        for j, w in enumerate((wk_ref, wv_ref)):
            fetches.append(pltpu.make_async_copy(w.at[at, :], to[j], sems.at[2 * i + j]))
    for fetch in fetches:
        fetch.start()
    for fetch in fetches[:3]:
        fetch.wait()
    req = owner_ref.shape[1]
    accepted = routes[0].astype(jnp.float32)
    owner = routes[1].astype(jnp.float32)
    page = routes[2].astype(jnp.float32)
    diagonal = iota((req, req), 0) == iota((req, req), 1)
    owner_col = jnp.sum(jnp.where(diagonal, owner, 0.0), axis=1, keepdims=True)
    earlier = (owner_col == owner) & (iota((req, req), 0) < iota((req, req), 1))
    within = jnp.sum(jnp.where(earlier, 1.0, 0.0), axis=0, keepdims=True)
    slot = owner * slot_cap + within
    row_count = req * draft
    lane, sub = iota((req, row_count), 1), iota((req, row_count), 0)
    mine = (lane >= sub * draft) & (lane < sub * draft + draft)
    slot_col = jnp.sum(jnp.where(diagonal, slot, 0.0), axis=1, keepdims=True)
    accepted_col = jnp.sum(jnp.where(diagonal, accepted, 0.0), axis=1, keepdims=True)
    draft_row = (lane - sub * draft).astype(jnp.float32)
    wanted = jnp.where(
        mine & (draft_row < accepted_col), slot_col * draft + draft_row + 1.0, 0.0
    )
    target = jnp.sum(wanted, axis=0, keepdims=True) - 1.0
    place = iota(select_ref.shape, 0).astype(jnp.float32)
    select_ref[...] = jnp.where(place == target, 1.0, 0.0).astype(jnp.bfloat16)
    part_lanes = head_cols // slot_cap
    dest = lax.div(iota((notes_ref.shape[0], req), 0), draft).astype(jnp.float32)
    note_lane = iota(notes_ref.shape, 1)
    notes = jnp.full(notes_ref.shape, -1.0, jnp.float32)
    for s in range(slot_cap):
        found = jnp.sum(
            jnp.where(dest * slot_cap + s == slot, page + 1.0, 0.0), axis=1, keepdims=True
        ) - 1.0
        notes = jnp.where(note_lane >= s * part_lanes, found, notes)
    notes_ref[...] = notes.astype(jnp.bfloat16)
    total = None
    for i in range(count):
        rows = jnp.concatenate([b[...] for b in blocks[i * CHUNKS : (i + 1) * CHUNKS]], axis=0)
        fetches[3 + 2 * i].wait()
        fetches[4 + 2 * i].wait()
        both = jnp.concatenate([weights[i, 0], weights[i, 1]], axis=1)
        part = jnp.dot(rows, both, preferred_element_type=jnp.float32)
        total = part if total is None else total + part
    total_ref[...] = total
    fetches[3 + 2 * count].wait()
    fetches[4 + 2 * count].wait()


def pack_kernel(slot_cap, draft, total_ref, lastk_ref, lastv_ref, select_ref, notes_ref, *refs):
    out_ref = refs[-1]
    rows = jnp.concatenate([b[...] for b in refs[:-1]], axis=0)
    both = jnp.concatenate([lastk_ref[...], lastv_ref[...]], axis=1)
    total = total_ref[...] + jnp.dot(rows, both, preferred_element_type=jnp.float32)
    packed = jnp.dot(
        select_ref[...], total.astype(jnp.bfloat16), preferred_element_type=jnp.float32
    ).astype(jnp.bfloat16)
    owners, _, head_cols = out_ref.shape
    span = slot_cap * draft
    out_ref[:, 0:span, :] = packed[:, :head_cols].reshape(owners, span, head_cols)
    out_ref[:, span : 2 * span, :] = packed[:, head_cols:].reshape(owners, span, head_cols)
    out_ref[:, 2 * span :, :] = notes_ref[...].reshape(owners, draft, head_cols)


def place_kernel(slot_cap, arrived_ref, key_ref, value_ref):
    sources, _, head_cols = arrived_ref.shape
    pages, draft, _ = key_ref.shape
    span = slot_cap * draft
    rows = sources * draft
    part_lanes = head_cols // slot_cap
    notes = arrived_ref[:, 2 * span :, :].reshape(rows, head_cols).astype(jnp.float32)
    draft_row = lax.rem(iota((rows, 1), 0), draft).astype(jnp.float32)
    spot = iota((rows, pages * draft), 1).astype(jnp.float32)
    total = None
    for s in range(slot_cap):
        page = notes[:, s * part_lanes : s * part_lanes + 1]
        goes = jnp.where(page >= 0.0, page * draft + draft_row, -1.0)
        select = jnp.where(goes == spot, 1.0, 0.0).astype(jnp.bfloat16)
        keys = arrived_ref[:, s * draft : (s + 1) * draft, :].reshape(rows, head_cols)
        values = arrived_ref[:, span + s * draft : span + (s + 1) * draft, :].reshape(rows, head_cols)
        both = jnp.concatenate([keys, values], axis=1)
        part = lax.dot_general(
            select, both, (((0,), (0,)), ((), ())), preferred_element_type=jnp.float32
        )
        total = part if total is None else total + part
    placed = total.astype(jnp.bfloat16)
    key_ref[...] = placed[:, :head_cols].reshape(pages, draft, head_cols)
    value_ref[...] = placed[:, head_cols:].reshape(pages, draft, head_cols)


def local(draft_features, w_key, w_value, accepted, owner_group, page_slot):
    req_dev = accepted.shape[0]
    draft = draft_features.shape[0] // req_dev
    depth = draft_features.shape[1]
    head_cols = w_key.shape[1]
    seq_count = lax.axis_size("seq")
    slot_cap = max(2, 2 * req_dev // seq_count)
    slot_total = slot_cap * seq_count
    routes = [a.reshape(1, req_dev) for a in (accepted, owner_group, page_slot)]
    me = lax.axis_index("head").astype(jnp.int32).reshape(1)
    held = gather_ring(draft_features)
    offsets = tuple(offset for offset, _ in held)
    blocks = [b for _, chunks in held for b in chunks]
    vmem = pl.BlockSpec(memory_space=pltpu.VMEM)
    hbm = pl.BlockSpec(memory_space=pltpu.HBM)
    early, late = blocks[:-CHUNKS], blocks[-CHUNKS:]
    row_count, heads = req_dev * draft, len(offsets)
    total, last_key, last_value, select, notes = pl.pallas_call(
        functools.partial(project_kernel, offsets, slot_cap, draft),
        out_shape=(
            jax.ShapeDtypeStruct((row_count, 2 * head_cols), jnp.float32),
            jax.ShapeDtypeStruct((depth, head_cols), jnp.bfloat16),
            jax.ShapeDtypeStruct((depth, head_cols), jnp.bfloat16),
            jax.ShapeDtypeStruct((slot_total * draft, row_count), jnp.bfloat16),
            jax.ShapeDtypeStruct((seq_count * draft, head_cols), jnp.bfloat16),
        ),
        in_specs=[pl.BlockSpec(memory_space=pltpu.SMEM)] + [hbm] * 5 + [vmem] * len(early),
        out_specs=(vmem,) * 5,
        scratch_shapes=[
            pltpu.VMEM((heads - 1, 2, depth, head_cols), jnp.bfloat16),
            pltpu.VMEM((3, 1, req_dev), jnp.int32),
            pltpu.SemaphoreType.DMA((2 * heads + 3,)),
        ],
        cost_estimate=pl.CostEstimate(
            flops=4 * row_count * depth * heads * head_cols,
            bytes_accessed=2 * (row_count + 2 * head_cols) * depth * heads,
            transcendentals=0,
        ),
        compiler_params=pltpu.CompilerParams(vmem_limit_bytes=PROJECT_VMEM),
        name="project",
    )(me, *routes, w_key, w_value, *early)
    packed = pl.pallas_call(
        functools.partial(pack_kernel, slot_cap, draft),
        out_shape=jax.ShapeDtypeStruct(
            (seq_count, 2 * slot_cap * draft + draft, head_cols), jnp.bfloat16
        ),
        in_specs=[vmem] * (5 + len(late)),
        out_specs=vmem,
        compiler_params=pltpu.CompilerParams(vmem_limit_bytes=OTHER_VMEM),
        name="pack",
    )(total, last_key, last_value, select, notes, *late)
    arrived = lax.all_to_all(packed, "seq", split_axis=0, concat_axis=0, tiled=True)
    cache = jax.ShapeDtypeStruct((slot_total, draft, head_cols), jnp.bfloat16)
    return pl.pallas_call(
        functools.partial(place_kernel, slot_cap),
        out_shape=(cache, cache),
        in_specs=[vmem],
        out_specs=(vmem, vmem),
        compiler_params=pltpu.CompilerParams(vmem_limit_bytes=OTHER_VMEM),
        name="place",
    )(arrived)


def solution(mesh):
    placed = (
        P(("grp", "seq"), "head"),
        P(None, "head"),
        P(None, "head"),
        P(("grp", "seq")),
        P(("grp", "seq")),
        P(("grp", "seq")),
    )
    return jax.shard_map(
        local,
        mesh=mesh,
        in_specs=placed,
        out_specs=(P(("grp", "seq"), None, "head"), P(("grp", "seq"), None, "head")),
        check_vma=False,
    )
```

```python
import functools

import jax
import jax.numpy as jnp
from jax import lax
from jax.experimental import pallas as pl
from jax.experimental.pallas import tpu as pltpu
from jax.sharding import PartitionSpec as P

CHUNKS = 2
PROJECT_VMEM = 50 * 2**20
OTHER_VMEM = 12 * 2**20


def gather_ring(block):
    heads, lines = lax.axis_size("head"), lax.axis_size("seq")

    def turn(step):
        return [
            (line * heads + i, line * heads + (i + (step if line % 2 == 0 else -step)) % heads)
            for line in range(lines)
            for i in range(heads)
        ]

    axes, up, down = ("seq", "head"), turn(1), turn(-1)
    own = jnp.split(block, CHUNKS, axis=0)
    held = [(0, own)]
    rising, falling = list(own), list(own)
    for step in range(1, (heads + 1) // 2):
        for c in range(CHUNKS):
            rising[c] = lax.ppermute(rising[c], axes, up)
            falling[c] = lax.ppermute(falling[c], axes, down)
        held.append((-step, list(rising)))
        held.append((step, list(falling)))
    if heads % 2 == 0:
        last = [
            lax.ppermute(rising[c], axes, up) if c % 2 == 0 else lax.ppermute(falling[c], axes, down)
            for c in range(CHUNKS)
        ]
        held.append((heads // 2, last))
    return held


def iota(shape, dim):
    return lax.broadcasted_iota(jnp.int32, shape, dim)


def project_kernel(offsets, slot_cap, draft, me_ref, accepted_ref, owner_ref, page_ref, wk_ref, wv_ref, *refs):
    count = len(offsets) - 1
    blocks = refs[: count * CHUNKS]
    total_ref, lastk_ref, lastv_ref, select_ref, notes_ref, weights, sems = refs[count * CHUNKS :]
    depth, head_cols = blocks[0].shape[1], wk_ref.shape[1]
    heads = len(offsets)
    fetches = []
    for i, offset in enumerate(offsets):
        origin = lax.rem(me_ref[0] + me_ref[1] * offset + heads, heads)
        at = pl.ds(pl.multiple_of(origin * depth, depth), depth)
        to = (weights.at[i, 0], weights.at[i, 1]) if i < count else (lastk_ref, lastv_ref)
        for j, w in enumerate((wk_ref, wv_ref)):
            fetches.append(pltpu.make_async_copy(w.at[at, :], to[j], sems.at[2 * i + j]))
    for fetch in fetches:
        fetch.start()
    req = owner_ref.shape[0]
    spot = iota((1, req), 1)
    accepted = owner = page = jnp.zeros((1, req), jnp.int32)
    for r in range(req):
        accepted = jnp.where(spot == r, accepted_ref[r], accepted)
        owner = jnp.where(spot == r, owner_ref[r], owner)
        page = jnp.where(spot == r, page_ref[r], page)
    accepted, owner, page = (a.astype(jnp.float32) for a in (accepted, owner, page))
    diagonal = iota((req, req), 0) == iota((req, req), 1)
    owner_col = jnp.sum(jnp.where(diagonal, owner, 0.0), axis=1, keepdims=True)
    earlier = (owner_col == owner) & (iota((req, req), 0) < iota((req, req), 1))
    within = jnp.sum(jnp.where(earlier, 1.0, 0.0), axis=0, keepdims=True)
    slot = owner * slot_cap + within
    row_count = req * draft
    lane, sub = iota((req, row_count), 1), iota((req, row_count), 0)
    mine = (lane >= sub * draft) & (lane < sub * draft + draft)
    slot_col = jnp.sum(jnp.where(diagonal, slot, 0.0), axis=1, keepdims=True)
    accepted_col = jnp.sum(jnp.where(diagonal, accepted, 0.0), axis=1, keepdims=True)
    draft_row = (lane - sub * draft).astype(jnp.float32)
    wanted = jnp.where(
        mine & (draft_row < accepted_col), slot_col * draft + draft_row + 1.0, 0.0
    )
    target = jnp.sum(wanted, axis=0, keepdims=True) - 1.0
    row = iota(select_ref.shape, 0).astype(jnp.float32)
    select_ref[...] = jnp.where(row == target, 1.0, 0.0).astype(jnp.bfloat16)
    taken = iota((notes_ref.shape[0], req), 0).astype(jnp.float32) == slot
    found = jnp.sum(jnp.where(taken, page + 1.0, 0.0), axis=1, keepdims=True)
    notes_ref[...] = jnp.broadcast_to(found, notes_ref.shape).astype(jnp.bfloat16)
    total = None
    for i in range(count):
        rows = jnp.concatenate([b[...] for b in blocks[i * CHUNKS : (i + 1) * CHUNKS]], axis=0)
        fetches[2 * i].wait()
        fetches[2 * i + 1].wait()
        both = jnp.concatenate([weights[i, 0], weights[i, 1]], axis=1)
        part = jnp.dot(rows, both, preferred_element_type=jnp.float32)
        total = part if total is None else total + part
    total_ref[...] = total
    fetches[2 * count].wait()
    fetches[2 * count + 1].wait()


def pack_kernel(slot_cap, draft, total_ref, lastk_ref, lastv_ref, select_ref, notes_ref, *refs):
    out_ref = refs[-1]
    rows = jnp.concatenate([b[...] for b in refs[:-1]], axis=0)
    both = jnp.concatenate([lastk_ref[...], lastv_ref[...]], axis=1)
    total = total_ref[...] + jnp.dot(rows, both, preferred_element_type=jnp.float32)
    packed = jnp.dot(
        select_ref[...], total.astype(jnp.bfloat16), preferred_element_type=jnp.float32
    ).astype(jnp.bfloat16)
    head_cols = out_ref.shape[1]
    span = slot_cap * draft
    stride = 2 * span + slot_cap
    for d in range(out_ref.shape[0] // stride):
        at = d * stride
        out_ref[at : at + span, :] = packed[d * span : (d + 1) * span, :head_cols]
        out_ref[at + span : at + 2 * span, :] = packed[d * span : (d + 1) * span, head_cols:]
        out_ref[at + 2 * span : at + stride, :] = notes_ref[d * slot_cap : (d + 1) * slot_cap, :]


def place_kernel(slot_cap, arrived_ref, key_ref, value_ref, rows_ref, notes_ref):
    pages, draft, head_cols = key_ref.shape
    span = slot_cap * draft
    stride = 2 * span + slot_cap
    sources = arrived_ref.shape[0] // stride
    rows = sources * draft
    for d in range(sources):
        rows_ref[d] = arrived_ref[d * stride : d * stride + 2 * span, :]
        notes = arrived_ref[d * stride + 2 * span : (d + 1) * stride, :].astype(jnp.float32)
        for s in range(slot_cap):
            notes_ref[s, d * draft : (d + 1) * draft, :] = jnp.broadcast_to(
                notes[s : s + 1, :], (draft, head_cols)
            )
    draft_row = lax.rem(iota((rows, head_cols), 0), draft).astype(jnp.float32)
    total = None
    for s in range(slot_cap):
        page = notes_ref[s]
        goes = jnp.where(page > 0.0, (page - 1.0) * draft + draft_row, -1.0)
        select = jnp.concatenate(
            [
                jnp.where(goes == (iota(goes.shape, 1) + at).astype(jnp.float32), 1.0, 0.0)
                for at in range(0, pages * draft, head_cols)
            ],
            axis=1,
        ).astype(jnp.bfloat16)
        keys = rows_ref[:, s * draft : (s + 1) * draft, :].reshape(rows, head_cols)
        values = rows_ref[:, span + s * draft : span + (s + 1) * draft, :].reshape(rows, head_cols)
        both = jnp.concatenate([keys, values], axis=1)
        part = lax.dot_general(
            select, both, (((0,), (0,)), ((), ())), preferred_element_type=jnp.float32
        )
        total = part if total is None else total + part
    placed = total.astype(jnp.bfloat16)
    key_ref[...] = placed[:, :head_cols].reshape(pages, draft, head_cols)
    value_ref[...] = placed[:, head_cols:].reshape(pages, draft, head_cols)


def local(draft_features, w_key, w_value, accepted, owner_group, page_slot):
    req_dev = accepted.shape[0]
    draft = draft_features.shape[0] // req_dev
    depth = draft_features.shape[1]
    head_cols = w_key.shape[1]
    seq_count = lax.axis_size("seq")
    slot_cap = max(2, 2 * req_dev // seq_count)
    slot_total = slot_cap * seq_count
    turn = 1 - 2 * lax.rem(lax.axis_index("seq"), 2)
    me = jnp.stack([lax.axis_index("head"), turn]).astype(jnp.int32)
    held = gather_ring(draft_features)
    offsets = tuple(offset for offset, _ in held)
    blocks = [b for _, chunks in held for b in chunks]
    vmem = pl.BlockSpec(memory_space=pltpu.VMEM)
    hbm = pl.BlockSpec(memory_space=pltpu.HBM)
    smem = pl.BlockSpec(memory_space=pltpu.SMEM)
    early, late = blocks[:-CHUNKS], blocks[-CHUNKS:]
    row_count, heads = req_dev * draft, len(offsets)
    stride = 2 * slot_cap * draft + slot_cap
    total, last_key, last_value, select, notes = pl.pallas_call(
        functools.partial(project_kernel, offsets, slot_cap, draft),
        out_shape=(
            jax.ShapeDtypeStruct((row_count, 2 * head_cols), jnp.float32),
            jax.ShapeDtypeStruct((depth, head_cols), jnp.bfloat16),
            jax.ShapeDtypeStruct((depth, head_cols), jnp.bfloat16),
            jax.ShapeDtypeStruct((slot_total * draft, row_count), jnp.bfloat16),
            jax.ShapeDtypeStruct((slot_total, head_cols), jnp.bfloat16),
        ),
        in_specs=[smem] * 4 + [hbm] * 2 + [vmem] * len(early),
        out_specs=(vmem,) * 5,
        scratch_shapes=[
            pltpu.VMEM((heads - 1, 2, depth, head_cols), jnp.bfloat16),
            pltpu.SemaphoreType.DMA((2 * heads,)),
        ],
        cost_estimate=pl.CostEstimate(
            flops=4 * row_count * depth * heads * head_cols,
            bytes_accessed=2 * (row_count + 2 * head_cols) * depth * heads,
            transcendentals=0,
        ),
        compiler_params=pltpu.CompilerParams(vmem_limit_bytes=PROJECT_VMEM),
        name="project",
    )(me, accepted, owner_group, page_slot, w_key, w_value, *early)
    packed = pl.pallas_call(
        functools.partial(pack_kernel, slot_cap, draft),
        out_shape=jax.ShapeDtypeStruct((seq_count * stride, head_cols), jnp.bfloat16),
        in_specs=[vmem] * (5 + len(late)),
        out_specs=vmem,
        compiler_params=pltpu.CompilerParams(vmem_limit_bytes=OTHER_VMEM),
        name="pack",
    )(total, last_key, last_value, select, notes, *late)
    paired = packed.reshape(seq_count, stride // 2, 2, head_cols)
    arrived = lax.all_to_all(paired, "seq", split_axis=0, concat_axis=0, tiled=True).reshape(packed.shape)
    cache = jax.ShapeDtypeStruct((slot_total, draft, head_cols), jnp.bfloat16)
    return pl.pallas_call(
        functools.partial(place_kernel, slot_cap),
        out_shape=(cache, cache),
        in_specs=[vmem],
        out_specs=(vmem, vmem),
        scratch_shapes=[
            pltpu.VMEM((seq_count, 2 * slot_cap * draft, head_cols), jnp.bfloat16),
            pltpu.VMEM((slot_cap, seq_count * draft, head_cols), jnp.float32),
        ],
        compiler_params=pltpu.CompilerParams(vmem_limit_bytes=OTHER_VMEM),
        name="place",
    )(arrived)


def solution(mesh):
    placed = (
        P(("grp", "seq"), "head"),
        P(None, "head"),
        P(None, "head"),
        P(("grp", "seq")),
        P(("grp", "seq")),
        P(("grp", "seq")),
    )
    return jax.shard_map(
        local,
        mesh=mesh,
        in_specs=placed,
        out_specs=(P(("grp", "seq"), None, "head"), P(("grp", "seq"), None, "head")),
        check_vma=False,
    )
```

```python
import functools

import jax
import jax.numpy as jnp
from jax import lax
from jax.experimental import pallas as pl
from jax.experimental.pallas import tpu as pltpu
from jax.sharding import PartitionSpec as P

CHUNKS = 2
PROJECT_VMEM = 49 * 2**20
OTHER_VMEM = 12 * 2**20


def gather_ring(block):
    heads, lines = lax.axis_size("head"), lax.axis_size("seq")

    def turn(step):
        return [
            (line * heads + i, line * heads + (i + (step if line % 2 == 0 else -step)) % heads)
            for line in range(lines)
            for i in range(heads)
        ]

    axes, up, down = ("seq", "head"), turn(1), turn(-1)
    own = jnp.split(block, CHUNKS, axis=0)
    held = [(0, own)]
    rising, falling = list(own), list(own)
    for step in range(1, (heads + 1) // 2):
        for c in range(CHUNKS):
            rising[c] = lax.ppermute(rising[c], axes, up)
            falling[c] = lax.ppermute(falling[c], axes, down)
        held.append((-step, list(rising)))
        held.append((step, list(falling)))
    if heads % 2 == 0:
        last = [
            lax.ppermute(rising[c], axes, up) if c % 2 == 0 else lax.ppermute(falling[c], axes, down)
            for c in range(CHUNKS)
        ]
        held.append((heads // 2, last))
    return held


def iota(shape, dim):
    return lax.broadcasted_iota(jnp.int32, shape, dim)


def project_kernel(offsets, slot_cap, draft, owners, me_ref, turn_ref, route_ref, wk_ref, wv_ref, *refs):
    count = len(offsets) - 1
    blocks = refs[: count * CHUNKS]
    total_ref, lastk_ref, lastv_ref, select_ref, notes_ref, weights, sems = refs[count * CHUNKS :]
    depth, head_cols = blocks[0].shape[1], wk_ref.shape[1]
    heads = len(offsets)
    fetches = []
    for i, offset in enumerate(offsets):
        origin = lax.rem(me_ref[0] + turn_ref[0] * offset + heads, heads)
        at = pl.ds(pl.multiple_of(origin * depth, depth), depth)
        to = (weights.at[i, 0], weights.at[i, 1]) if i < count else (lastk_ref, lastv_ref)
        for j, w in enumerate((wk_ref, wv_ref)):
            fetches.append(pltpu.make_async_copy(w.at[at, :], to[j], sems.at[2 * i + j]))
    for fetch in fetches:
        fetch.start()
    req = route_ref.shape[1]
    slots = owners * slot_cap
    route = route_ref[...]
    page = lax.rem(route, slots).astype(jnp.float32)
    owner = lax.rem(lax.div(route, slots), owners).astype(jnp.float32)
    accepted = lax.div(route, slots * owners).astype(jnp.float32)
    diagonal = iota((req, req), 0) == iota((req, req), 1)
    owner_col = jnp.sum(jnp.where(diagonal, owner, 0.0), axis=1, keepdims=True)
    earlier = (owner_col == owner) & (iota((req, req), 0) < iota((req, req), 1))
    within = jnp.sum(jnp.where(earlier, 1.0, 0.0), axis=0, keepdims=True)
    slot = owner * slot_cap + within
    row_count = req * draft
    lane, sub = iota((req, row_count), 1), iota((req, row_count), 0)
    mine = (lane >= sub * draft) & (lane < sub * draft + draft)
    slot_col = jnp.sum(jnp.where(diagonal, slot, 0.0), axis=1, keepdims=True)
    accepted_col = jnp.sum(jnp.where(diagonal, accepted, 0.0), axis=1, keepdims=True)
    draft_row = (lane - sub * draft).astype(jnp.float32)
    wanted = jnp.where(
        mine & (draft_row < accepted_col), slot_col * draft + draft_row + 1.0, 0.0
    )
    target = jnp.sum(wanted, axis=0, keepdims=True) - 1.0
    row = iota(select_ref.shape, 0).astype(jnp.float32)
    select_ref[...] = jnp.where(row == target, 1.0, 0.0).astype(jnp.bfloat16)
    taken = iota((notes_ref.shape[0], req), 0).astype(jnp.float32) == slot
    found = jnp.sum(jnp.where(taken, page + 1.0, 0.0), axis=1, keepdims=True)
    notes_ref[...] = jnp.broadcast_to(found, notes_ref.shape).astype(jnp.bfloat16)
    total = None
    for i in range(count):
        rows = jnp.concatenate([b[...] for b in blocks[i * CHUNKS : (i + 1) * CHUNKS]], axis=0)
        fetches[2 * i].wait()
        fetches[2 * i + 1].wait()
        both = jnp.concatenate([weights[i, 0], weights[i, 1]], axis=1)
        part = jnp.dot(rows, both, preferred_element_type=jnp.float32)
        total = part if total is None else total + part
    total_ref[...] = total
    fetches[2 * count].wait()
    fetches[2 * count + 1].wait()


def pack_kernel(slot_cap, draft, total_ref, lastk_ref, lastv_ref, select_ref, notes_ref, *refs):
    out_ref = refs[-1]
    rows = jnp.concatenate([b[...] for b in refs[:-1]], axis=0)
    both = jnp.concatenate([lastk_ref[...], lastv_ref[...]], axis=1)
    total = total_ref[...] + jnp.dot(rows, both, preferred_element_type=jnp.float32)
    packed = jnp.dot(
        select_ref[...], total.astype(jnp.bfloat16), preferred_element_type=jnp.float32
    ).astype(jnp.bfloat16)
    head_cols = out_ref.shape[1]
    span = slot_cap * draft
    stride = 2 * span + slot_cap
    for d in range(out_ref.shape[0] // stride):
        at = d * stride
        out_ref[at : at + span, :] = packed[d * span : (d + 1) * span, :head_cols]
        out_ref[at + span : at + 2 * span, :] = packed[d * span : (d + 1) * span, head_cols:]
        out_ref[at + 2 * span : at + stride, :] = notes_ref[d * slot_cap : (d + 1) * slot_cap, :]


def place_kernel(slot_cap, arrived_ref, key_ref, value_ref, rows_ref, notes_ref):
    pages, draft, head_cols = key_ref.shape
    span = slot_cap * draft
    stride = 2 * span + slot_cap
    sources = arrived_ref.shape[0] // stride
    rows = sources * draft
    for d in range(sources):
        rows_ref[d] = arrived_ref[d * stride : d * stride + 2 * span, :]
        notes = arrived_ref[d * stride + 2 * span : (d + 1) * stride, :].astype(jnp.float32)
        for s in range(slot_cap):
            notes_ref[s, d * draft : (d + 1) * draft, :] = jnp.broadcast_to(
                notes[s : s + 1, :], (draft, head_cols)
            )
    draft_row = lax.rem(iota((rows, head_cols), 0), draft).astype(jnp.float32)
    total = None
    for s in range(slot_cap):
        page = notes_ref[s]
        goes = jnp.where(page > 0.0, (page - 1.0) * draft + draft_row, -1.0)
        select = jnp.concatenate(
            [
                jnp.where(goes == (iota(goes.shape, 1) + at).astype(jnp.float32), 1.0, 0.0)
                for at in range(0, pages * draft, head_cols)
            ],
            axis=1,
        ).astype(jnp.bfloat16)
        keys = rows_ref[:, s * draft : (s + 1) * draft, :].reshape(rows, head_cols)
        values = rows_ref[:, span + s * draft : span + (s + 1) * draft, :].reshape(rows, head_cols)
        both = jnp.concatenate([keys, values], axis=1)
        part = lax.dot_general(
            select, both, (((0,), (0,)), ((), ())), preferred_element_type=jnp.float32
        )
        total = part if total is None else total + part
    placed = total.astype(jnp.bfloat16)
    key_ref[...] = placed[:, :head_cols].reshape(pages, draft, head_cols)
    value_ref[...] = placed[:, head_cols:].reshape(pages, draft, head_cols)


def local(draft_features, w_key, w_value, accepted, owner_group, page_slot):
    req_dev = accepted.shape[0]
    draft = draft_features.shape[0] // req_dev
    depth = draft_features.shape[1]
    head_cols = w_key.shape[1]
    seq_count = lax.axis_size("seq")
    slot_cap = max(2, 2 * req_dev // seq_count)
    slot_total = slot_cap * seq_count
    me = lax.axis_index("head").astype(jnp.int32).reshape(1)
    turn = (1 - 2 * (lax.axis_index("seq") & 1)).astype(jnp.int32).reshape(1)
    route = ((accepted * seq_count + owner_group) * slot_total + page_slot).reshape(1, req_dev)
    held = gather_ring(draft_features)
    offsets = tuple(offset for offset, _ in held)
    blocks = [b for _, chunks in held for b in chunks]
    vmem = pl.BlockSpec(memory_space=pltpu.VMEM)
    hbm = pl.BlockSpec(memory_space=pltpu.HBM)
    smem = pl.BlockSpec(memory_space=pltpu.SMEM)
    early, late = blocks[:-CHUNKS], blocks[-CHUNKS:]
    row_count, heads = req_dev * draft, len(offsets)
    stride = 2 * slot_cap * draft + slot_cap
    total, last_key, last_value, select, notes = pl.pallas_call(
        functools.partial(project_kernel, offsets, slot_cap, draft, seq_count),
        out_shape=(
            jax.ShapeDtypeStruct((row_count, 2 * head_cols), jnp.float32),
            jax.ShapeDtypeStruct((depth, head_cols), jnp.bfloat16),
            jax.ShapeDtypeStruct((depth, head_cols), jnp.bfloat16),
            jax.ShapeDtypeStruct((slot_total * draft, row_count), jnp.bfloat16),
            jax.ShapeDtypeStruct((slot_total, head_cols), jnp.bfloat16),
        ),
        in_specs=[smem, smem, vmem] + [hbm] * 2 + [vmem] * len(early),
        out_specs=(vmem,) * 5,
        scratch_shapes=[
            pltpu.VMEM((heads - 1, 2, depth, head_cols), jnp.bfloat16),
            pltpu.SemaphoreType.DMA((2 * heads,)),
        ],
        cost_estimate=pl.CostEstimate(
            flops=4 * row_count * depth * heads * head_cols,
            bytes_accessed=2 * (row_count + 2 * head_cols) * depth * heads,
            transcendentals=0,
        ),
        compiler_params=pltpu.CompilerParams(vmem_limit_bytes=PROJECT_VMEM),
        name="project",
    )(me, turn, route, w_key, w_value, *early)
    packed = pl.pallas_call(
        functools.partial(pack_kernel, slot_cap, draft),
        out_shape=jax.ShapeDtypeStruct((seq_count * stride, head_cols), jnp.bfloat16),
        in_specs=[vmem] * (5 + len(late)),
        out_specs=vmem,
        compiler_params=pltpu.CompilerParams(vmem_limit_bytes=OTHER_VMEM),
        name="pack",
    )(total, last_key, last_value, select, notes, *late)
    paired = packed.reshape(seq_count, stride // 2, 2, head_cols)
    arrived = lax.all_to_all(paired, "seq", split_axis=0, concat_axis=0, tiled=True).reshape(packed.shape)
    cache = jax.ShapeDtypeStruct((slot_total, draft, head_cols), jnp.bfloat16)
    return pl.pallas_call(
        functools.partial(place_kernel, slot_cap),
        out_shape=(cache, cache),
        in_specs=[vmem],
        out_specs=(vmem, vmem),
        scratch_shapes=[
            pltpu.VMEM((seq_count, 2 * slot_cap * draft, head_cols), jnp.bfloat16),
            pltpu.VMEM((slot_cap, seq_count * draft, head_cols), jnp.float32),
        ],
        compiler_params=pltpu.CompilerParams(vmem_limit_bytes=OTHER_VMEM),
        name="place",
    )(arrived)


def solution(mesh):
    placed = (
        P(("grp", "seq"), "head"),
        P(None, "head"),
        P(None, "head"),
        P(("grp", "seq")),
        P(("grp", "seq")),
        P(("grp", "seq")),
    )
    return jax.shard_map(
        local,
        mesh=mesh,
        in_specs=placed,
        out_specs=(P(("grp", "seq"), None, "head"), P(("grp", "seq"), None, "head")),
        check_vma=False,
    )
```

```python
import functools

import jax
import jax.numpy as jnp
from jax import lax
from jax.experimental import pallas as pl
from jax.experimental.pallas import tpu as pltpu
from jax.sharding import PartitionSpec as P

CHUNKS = 2
PROJECT_VMEM = 49 * 2**20
OTHER_VMEM = 12 * 2**20


def gather_ring(block):
    heads, lines = lax.axis_size("head"), lax.axis_size("seq")

    def turn(step):
        return [
            (line * heads + i, line * heads + (i + (step if line % 2 == 0 else -step)) % heads)
            for line in range(lines)
            for i in range(heads)
        ]

    axes, up, down = ("seq", "head"), turn(1), turn(-1)
    own = jnp.split(block, CHUNKS, axis=0)
    held = [(0, own)]
    rising, falling = list(own), list(own)
    for step in range(1, (heads + 1) // 2):
        for c in range(CHUNKS):
            rising[c] = lax.ppermute(rising[c], axes, up)
            falling[c] = lax.ppermute(falling[c], axes, down)
        held.append((-step, list(rising)))
        held.append((step, list(falling)))
    if heads % 2 == 0:
        last = [
            lax.ppermute(rising[c], axes, up) if c % 2 == 0 else lax.ppermute(falling[c], axes, down)
            for c in range(CHUNKS)
        ]
        held.append((heads // 2, last))
    return held


def iota(shape, dim):
    return lax.broadcasted_iota(jnp.int32, shape, dim)


def project_kernel(offsets, slot_cap, draft, owners, me_ref, turn_ref, route_ref, wk_ref, wv_ref, *refs):
    count = len(offsets) - 1
    blocks = refs[: count * CHUNKS]
    total_ref, lastk_ref, lastv_ref, select_ref, notes_ref, weights, sems = refs[count * CHUNKS :]
    depth, head_cols = blocks[0].shape[1], wk_ref.shape[1]
    heads = len(offsets)
    fetches = []
    for i, offset in enumerate(offsets):
        origin = lax.rem(me_ref[0] + turn_ref[0] * offset + heads, heads)
        at = pl.ds(pl.multiple_of(origin * depth, depth), depth)
        to = (weights.at[i, 0], weights.at[i, 1]) if i < count else (lastk_ref, lastv_ref)
        for j, w in enumerate((wk_ref, wv_ref)):
            fetches.append(pltpu.make_async_copy(w.at[at, :], to[j], sems.at[2 * i + j]))
    for fetch in fetches:
        fetch.start()
    req = route_ref.shape[1]
    slots = owners * slot_cap
    route = route_ref[...]
    page = lax.rem(route, slots).astype(jnp.float32)
    owner = lax.rem(lax.div(route, slots), owners).astype(jnp.float32)
    accepted = lax.div(route, slots * owners).astype(jnp.float32)
    diagonal = iota((req, req), 0) == iota((req, req), 1)
    owner_col = jnp.sum(jnp.where(diagonal, owner, 0.0), axis=1, keepdims=True)
    earlier = (owner_col == owner) & (iota((req, req), 0) < iota((req, req), 1))
    within = jnp.sum(jnp.where(earlier, 1.0, 0.0), axis=0, keepdims=True)
    slot = owner * slot_cap + within
    row_count = req * draft
    lane, sub = iota((req, row_count), 1), iota((req, row_count), 0)
    mine = (lane >= sub * draft) & (lane < sub * draft + draft)
    slot_col = jnp.sum(jnp.where(diagonal, slot, 0.0), axis=1, keepdims=True)
    accepted_col = jnp.sum(jnp.where(diagonal, accepted, 0.0), axis=1, keepdims=True)
    draft_row = (lane - sub * draft).astype(jnp.float32)
    wanted = jnp.where(
        mine & (draft_row < accepted_col), slot_col * draft + draft_row + 1.0, 0.0
    )
    target = jnp.sum(wanted, axis=0, keepdims=True) - 1.0
    row = iota(select_ref.shape, 0).astype(jnp.float32)
    select_ref[...] = jnp.where(row == target, 1.0, 0.0).astype(jnp.bfloat16)
    taken = iota((notes_ref.shape[0], req), 0).astype(jnp.float32) == slot
    found = jnp.sum(jnp.where(taken, page + 1.0, 0.0), axis=1, keepdims=True)
    notes_ref[...] = jnp.broadcast_to(found, notes_ref.shape).astype(jnp.bfloat16)
    total = None
    for i in range(count):
        rows = jnp.concatenate([b[...] for b in blocks[i * CHUNKS : (i + 1) * CHUNKS]], axis=0)
        fetches[2 * i].wait()
        fetches[2 * i + 1].wait()
        both = jnp.concatenate([weights[i, 0], weights[i, 1]], axis=1)
        part = jnp.dot(rows, both, preferred_element_type=jnp.float32)
        total = part if total is None else total + part
    total_ref[...] = total
    fetches[2 * count].wait()
    fetches[2 * count + 1].wait()


def pack_kernel(slot_cap, draft, total_ref, lastk_ref, lastv_ref, select_ref, notes_ref, *refs):
    out_ref = refs[-1]
    rows = jnp.concatenate([b[...] for b in refs[:-1]], axis=0)
    both = jnp.concatenate([lastk_ref[...], lastv_ref[...]], axis=1)
    total = total_ref[...] + jnp.dot(rows, both, preferred_element_type=jnp.float32)
    packed = jnp.dot(
        select_ref[...], total.astype(jnp.bfloat16), preferred_element_type=jnp.float32
    ).astype(jnp.bfloat16)
    head_cols = out_ref.shape[1]
    span = slot_cap * draft
    stride = 2 * span + slot_cap
    for d in range(out_ref.shape[0] // stride):
        at = d * stride
        out_ref[at : at + span, :] = packed[d * span : (d + 1) * span, :head_cols]
        out_ref[at + span : at + 2 * span, :] = packed[d * span : (d + 1) * span, head_cols:]
        out_ref[at + 2 * span : at + stride, :] = notes_ref[d * slot_cap : (d + 1) * slot_cap, :]


def place_kernel(slot_cap, side_ref, own_ref, other_ref, key_ref, value_ref, rows_ref, notes_ref):
    pages, draft, head_cols = key_ref.shape
    span = slot_cap * draft
    stride = 2 * span + slot_cap
    sources = rows_ref.shape[0]
    rows = sources * draft

    def take(side):
        for d in range(sources):
            from_ref = own_ref if 2 * d < sources else other_ref
            at = (2 * (d % (sources // 2)) + side) * stride
            rows_ref[d] = from_ref[at : at + 2 * span, :]
            notes = from_ref[at + 2 * span : at + stride, :].astype(jnp.float32)
            for s in range(slot_cap):
                notes_ref[s, d * draft : (d + 1) * draft, :] = jnp.broadcast_to(
                    notes[s : s + 1, :], (draft, head_cols)
                )

    for side in range(2):
        pl.when(side_ref[0] == side)(functools.partial(take, side))
    draft_row = lax.rem(iota((rows, head_cols), 0), draft).astype(jnp.float32)
    total = None
    for s in range(slot_cap):
        page = notes_ref[s]
        goes = jnp.where(page > 0.0, (page - 1.0) * draft + draft_row, -1.0)
        select = jnp.concatenate(
            [
                jnp.where(goes == (iota(goes.shape, 1) + at).astype(jnp.float32), 1.0, 0.0)
                for at in range(0, pages * draft, head_cols)
            ],
            axis=1,
        ).astype(jnp.bfloat16)
        keys = rows_ref[:, s * draft : (s + 1) * draft, :].reshape(rows, head_cols)
        values = rows_ref[:, span + s * draft : span + (s + 1) * draft, :].reshape(rows, head_cols)
        both = jnp.concatenate([keys, values], axis=1)
        part = lax.dot_general(
            select, both, (((0,), (0,)), ((), ())), preferred_element_type=jnp.float32
        )
        total = part if total is None else total + part
    placed = total.astype(jnp.bfloat16)
    key_ref[...] = placed[:, :head_cols].reshape(pages, draft, head_cols)
    value_ref[...] = placed[:, head_cols:].reshape(pages, draft, head_cols)


def local(draft_features, w_key, w_value, accepted, owner_group, page_slot):
    req_dev = accepted.shape[0]
    draft = draft_features.shape[0] // req_dev
    depth = draft_features.shape[1]
    head_cols = w_key.shape[1]
    seq_count = lax.axis_size("seq")
    slot_cap = max(2, 2 * req_dev // seq_count)
    slot_total = slot_cap * seq_count
    me = lax.axis_index("head").astype(jnp.int32).reshape(1)
    side = (lax.axis_index("seq") & 1).astype(jnp.int32).reshape(1)
    turn = 1 - 2 * side
    route = ((accepted * seq_count + owner_group) * slot_total + page_slot).reshape(1, req_dev)
    held = gather_ring(draft_features)
    offsets = tuple(offset for offset, _ in held)
    blocks = [b for _, chunks in held for b in chunks]
    vmem = pl.BlockSpec(memory_space=pltpu.VMEM)
    hbm = pl.BlockSpec(memory_space=pltpu.HBM)
    smem = pl.BlockSpec(memory_space=pltpu.SMEM)
    early, late = blocks[:-CHUNKS], blocks[-CHUNKS:]
    row_count, heads = req_dev * draft, len(offsets)
    stride = 2 * slot_cap * draft + slot_cap
    total, last_key, last_value, select, notes = pl.pallas_call(
        functools.partial(project_kernel, offsets, slot_cap, draft, seq_count),
        out_shape=(
            jax.ShapeDtypeStruct((row_count, 2 * head_cols), jnp.float32),
            jax.ShapeDtypeStruct((depth, head_cols), jnp.bfloat16),
            jax.ShapeDtypeStruct((depth, head_cols), jnp.bfloat16),
            jax.ShapeDtypeStruct((slot_total * draft, row_count), jnp.bfloat16),
            jax.ShapeDtypeStruct((slot_total, head_cols), jnp.bfloat16),
        ),
        in_specs=[smem, smem, vmem] + [hbm] * 2 + [vmem] * len(early),
        out_specs=(vmem,) * 5,
        scratch_shapes=[
            pltpu.VMEM((heads - 1, 2, depth, head_cols), jnp.bfloat16),
            pltpu.SemaphoreType.DMA((2 * heads,)),
        ],
        cost_estimate=pl.CostEstimate(
            flops=4 * row_count * depth * heads * head_cols,
            bytes_accessed=2 * (row_count + 2 * head_cols) * depth * heads,
            transcendentals=0,
        ),
        compiler_params=pltpu.CompilerParams(vmem_limit_bytes=PROJECT_VMEM),
        name="project",
    )(me, turn, route, w_key, w_value, *early)
    packed = pl.pallas_call(
        functools.partial(pack_kernel, slot_cap, draft),
        out_shape=jax.ShapeDtypeStruct((seq_count * stride, head_cols), jnp.bfloat16),
        in_specs=[vmem] * (5 + len(late)),
        out_specs=vmem,
        compiler_params=pltpu.CompilerParams(vmem_limit_bytes=OTHER_VMEM),
        name="pack",
    )(total, last_key, last_value, select, notes, *late)
    paired = packed.reshape(seq_count // 2, stride, 2, head_cols)
    sides = [list(range(side, seq_count, 2)) for side in range(2)]
    arrived = lax.all_to_all(
        paired, "seq", split_axis=0, concat_axis=0, tiled=True, axis_index_groups=sides
    ).reshape(packed.shape)
    shared = lax.ppermute(arrived, "seq", [(i, i ^ 1) for i in range(seq_count)])
    cache = jax.ShapeDtypeStruct((slot_total, draft, head_cols), jnp.bfloat16)
    return pl.pallas_call(
        functools.partial(place_kernel, slot_cap),
        out_shape=(cache, cache),
        in_specs=[smem, vmem, vmem],
        out_specs=(vmem, vmem),
        scratch_shapes=[
            pltpu.VMEM((seq_count, 2 * slot_cap * draft, head_cols), jnp.bfloat16),
            pltpu.VMEM((slot_cap, seq_count * draft, head_cols), jnp.float32),
        ],
        compiler_params=pltpu.CompilerParams(vmem_limit_bytes=OTHER_VMEM),
        name="place",
    )(side, arrived, shared)


def solution(mesh):
    placed = (
        P(("grp", "seq"), "head"),
        P(None, "head"),
        P(None, "head"),
        P(("grp", "seq")),
        P(("grp", "seq")),
        P(("grp", "seq")),
    )
    return jax.shard_map(
        local,
        mesh=mesh,
        in_specs=placed,
        out_specs=(P(("grp", "seq"), None, "head"), P(("grp", "seq"), None, "head")),
        check_vma=False,
    )
```

```python
import functools

import jax
import jax.numpy as jnp
from jax import lax
from jax.experimental import pallas as pl
from jax.experimental.pallas import tpu as pltpu
from jax.sharding import PartitionSpec as P

CHUNKS = 2
PROJECT_VMEM = 49 * 2**20
OTHER_VMEM = 12 * 2**20


def gather_ring(block):
    heads, lines = lax.axis_size("head"), lax.axis_size("seq")

    def turn(step):
        return [
            (line * heads + i, line * heads + (i + (step if line % 2 == 0 else -step)) % heads)
            for line in range(lines)
            for i in range(heads)
        ]

    axes, up, down = ("seq", "head"), turn(1), turn(-1)
    own = jnp.split(block, CHUNKS, axis=0)
    held = [(0, own)]
    rising, falling = list(own), list(own)
    for step in range(1, (heads + 1) // 2):
        for c in range(CHUNKS):
            rising[c] = lax.ppermute(rising[c], axes, up)
            falling[c] = lax.ppermute(falling[c], axes, down)
        held.append((-step, list(rising)))
        held.append((step, list(falling)))
    if heads % 2 == 0:
        last = [
            lax.ppermute(rising[c], axes, up) if c % 2 == 0 else lax.ppermute(falling[c], axes, down)
            for c in range(CHUNKS)
        ]
        held.append((heads // 2, last))
    return held


def iota(shape, dim):
    return lax.broadcasted_iota(jnp.int32, shape, dim)


def project_kernel(offsets, slot_cap, draft, owners, me_ref, turn_ref, route_ref, wk_ref, wv_ref, *refs):
    count = len(offsets) - 1
    blocks = refs[: count * CHUNKS]
    total_ref, lastk_ref, lastv_ref, select_ref, notes_ref, weights, sems = refs[count * CHUNKS :]
    depth, head_cols = blocks[0].shape[1], wk_ref.shape[1]
    heads = len(offsets)
    fetches = []
    for i, offset in enumerate(offsets):
        origin = lax.rem(me_ref[0] + turn_ref[0] * offset + heads, heads)
        at = pl.ds(pl.multiple_of(origin * depth, depth), depth)
        to = (weights.at[i, 0], weights.at[i, 1]) if i < count else (lastk_ref, lastv_ref)
        for j, w in enumerate((wk_ref, wv_ref)):
            fetches.append(pltpu.make_async_copy(w.at[at, :], to[j], sems.at[2 * i + j]))
    for fetch in fetches:
        fetch.start()
    req = route_ref.shape[1]
    slots = owners * slot_cap
    route = route_ref[...]
    page = lax.rem(route, slots).astype(jnp.float32)
    owner = lax.rem(lax.div(route, slots), owners).astype(jnp.float32)
    accepted = lax.div(route, slots * owners).astype(jnp.float32)
    diagonal = iota((req, req), 0) == iota((req, req), 1)
    owner_col = jnp.sum(jnp.where(diagonal, owner, 0.0), axis=1, keepdims=True)
    earlier = (owner_col == owner) & (iota((req, req), 0) < iota((req, req), 1))
    within = jnp.sum(jnp.where(earlier, 1.0, 0.0), axis=0, keepdims=True)
    slot = owner * slot_cap + within
    row_count = req * draft
    lane, sub = iota((req, row_count), 1), iota((req, row_count), 0)
    mine = (lane >= sub * draft) & (lane < sub * draft + draft)
    slot_col = jnp.sum(jnp.where(diagonal, slot, 0.0), axis=1, keepdims=True)
    accepted_col = jnp.sum(jnp.where(diagonal, accepted, 0.0), axis=1, keepdims=True)
    draft_row = (lane - sub * draft).astype(jnp.float32)
    wanted = jnp.where(
        mine & (draft_row < accepted_col), slot_col * draft + draft_row + 1.0, 0.0
    )
    target = jnp.sum(wanted, axis=0, keepdims=True) - 1.0
    row = iota(select_ref.shape, 0).astype(jnp.float32)
    select_ref[...] = jnp.where(row == target, 1.0, 0.0).astype(jnp.bfloat16)
    taken = iota((notes_ref.shape[0], req), 0).astype(jnp.float32) == slot
    found = jnp.sum(jnp.where(taken, page + 1.0, 0.0), axis=1, keepdims=True)
    notes_ref[...] = jnp.broadcast_to(found, notes_ref.shape).astype(jnp.bfloat16)
    total = None
    for group in (range(count // 2), range(count // 2, count)):
        rows, both = [], []
        for i in group:
            fetches[2 * i].wait()
            fetches[2 * i + 1].wait()
            rows.append(
                jnp.concatenate([b[...] for b in blocks[i * CHUNKS : (i + 1) * CHUNKS]], axis=0)
            )
            both.append(jnp.concatenate([weights[i, 0], weights[i, 1]], axis=1))
        part = jnp.dot(
            jnp.concatenate(rows, axis=1),
            jnp.concatenate(both, axis=0),
            preferred_element_type=jnp.float32,
        )
        total = part if total is None else total + part
    total_ref[...] = total
    fetches[2 * count].wait()
    fetches[2 * count + 1].wait()


def pack_kernel(slot_cap, draft, total_ref, lastk_ref, lastv_ref, select_ref, notes_ref, *refs):
    out_ref = refs[-1]
    rows = jnp.concatenate([b[...] for b in refs[:-1]], axis=0)
    both = jnp.concatenate([lastk_ref[...], lastv_ref[...]], axis=1)
    total = total_ref[...] + jnp.dot(rows, both, preferred_element_type=jnp.float32)
    packed = jnp.dot(
        select_ref[...], total.astype(jnp.bfloat16), preferred_element_type=jnp.float32
    ).astype(jnp.bfloat16)
    head_cols = out_ref.shape[1]
    span = slot_cap * draft
    stride = 2 * span + slot_cap
    for d in range(out_ref.shape[0] // stride):
        at = d * stride
        out_ref[at : at + span, :] = packed[d * span : (d + 1) * span, :head_cols]
        out_ref[at + span : at + 2 * span, :] = packed[d * span : (d + 1) * span, head_cols:]
        out_ref[at + 2 * span : at + stride, :] = notes_ref[d * slot_cap : (d + 1) * slot_cap, :]


def place_part(slot_cap, draft, pages, side_ref, from_ref, rows_ref, notes_ref):
    head_cols = from_ref.shape[1]
    span = slot_cap * draft
    stride = 2 * span + slot_cap
    sources = rows_ref.shape[0]
    rows = sources * draft

    def take(side):
        for d in range(sources):
            at = (2 * d + side) * stride
            rows_ref[d] = from_ref[at : at + 2 * span, :]
            notes = from_ref[at + 2 * span : at + stride, :].astype(jnp.float32)
            for s in range(slot_cap):
                notes_ref[s, d * draft : (d + 1) * draft, :] = jnp.broadcast_to(
                    notes[s : s + 1, :], (draft, head_cols)
                )

    for side in range(2):
        pl.when(side_ref[0] == side)(functools.partial(take, side))
    draft_row = lax.rem(iota((rows, head_cols), 0), draft).astype(jnp.float32)
    total = None
    for s in range(slot_cap):
        page = notes_ref[s]
        goes = jnp.where(page > 0.0, (page - 1.0) * draft + draft_row, -1.0)
        select = jnp.concatenate(
            [
                jnp.where(goes == (iota(goes.shape, 1) + at).astype(jnp.float32), 1.0, 0.0)
                for at in range(0, pages * draft, head_cols)
            ],
            axis=1,
        ).astype(jnp.bfloat16)
        keys = rows_ref[:, s * draft : (s + 1) * draft, :].reshape(rows, head_cols)
        values = rows_ref[:, span + s * draft : span + (s + 1) * draft, :].reshape(rows, head_cols)
        both = jnp.concatenate([keys, values], axis=1)
        part = lax.dot_general(
            select, both, (((0,), (0,)), ((), ())), preferred_element_type=jnp.float32
        )
        total = part if total is None else total + part
    return total


def place_own_kernel(slot_cap, draft, pages, side_ref, own_ref, total_ref, rows_ref, notes_ref):
    total_ref[...] = place_part(slot_cap, draft, pages, side_ref, own_ref, rows_ref, notes_ref)


def place_kernel(slot_cap, side_ref, total_ref, other_ref, key_ref, value_ref, rows_ref, notes_ref):
    pages, draft, head_cols = key_ref.shape
    part = place_part(slot_cap, draft, pages, side_ref, other_ref, rows_ref, notes_ref)
    placed = (total_ref[...] + part).astype(jnp.bfloat16)
    key_ref[...] = placed[:, :head_cols].reshape(pages, draft, head_cols)
    value_ref[...] = placed[:, head_cols:].reshape(pages, draft, head_cols)


def local(draft_features, w_key, w_value, accepted, owner_group, page_slot):
    req_dev = accepted.shape[0]
    draft = draft_features.shape[0] // req_dev
    depth = draft_features.shape[1]
    head_cols = w_key.shape[1]
    seq_count = lax.axis_size("seq")
    slot_cap = max(2, 2 * req_dev // seq_count)
    slot_total = slot_cap * seq_count
    me = lax.axis_index("head").astype(jnp.int32).reshape(1)
    side = (lax.axis_index("seq") & 1).astype(jnp.int32).reshape(1)
    turn = 1 - 2 * side
    route = ((accepted * seq_count + owner_group) * slot_total + page_slot).reshape(1, req_dev)
    held = gather_ring(draft_features)
    offsets = tuple(offset for offset, _ in held)
    blocks = [b for _, chunks in held for b in chunks]
    vmem = pl.BlockSpec(memory_space=pltpu.VMEM)
    hbm = pl.BlockSpec(memory_space=pltpu.HBM)
    smem = pl.BlockSpec(memory_space=pltpu.SMEM)
    early, late = blocks[:-CHUNKS], blocks[-CHUNKS:]
    row_count, heads = req_dev * draft, len(offsets)
    stride = 2 * slot_cap * draft + slot_cap
    total, last_key, last_value, select, notes = pl.pallas_call(
        functools.partial(project_kernel, offsets, slot_cap, draft, seq_count),
        out_shape=(
            jax.ShapeDtypeStruct((row_count, 2 * head_cols), jnp.float32),
            jax.ShapeDtypeStruct((depth, head_cols), jnp.bfloat16),
            jax.ShapeDtypeStruct((depth, head_cols), jnp.bfloat16),
            jax.ShapeDtypeStruct((slot_total * draft, row_count), jnp.bfloat16),
            jax.ShapeDtypeStruct((slot_total, head_cols), jnp.bfloat16),
        ),
        in_specs=[smem, smem, vmem] + [hbm] * 2 + [vmem] * len(early),
        out_specs=(vmem,) * 5,
        scratch_shapes=[
            pltpu.VMEM((heads - 1, 2, depth, head_cols), jnp.bfloat16),
            pltpu.SemaphoreType.DMA((2 * heads,)),
        ],
        cost_estimate=pl.CostEstimate(
            flops=4 * row_count * depth * heads * head_cols,
            bytes_accessed=2 * (row_count + 2 * head_cols) * depth * heads,
            transcendentals=0,
        ),
        compiler_params=pltpu.CompilerParams(vmem_limit_bytes=PROJECT_VMEM),
        name="project",
    )(me, turn, route, w_key, w_value, *early)
    packed = pl.pallas_call(
        functools.partial(pack_kernel, slot_cap, draft),
        out_shape=jax.ShapeDtypeStruct((seq_count * stride, head_cols), jnp.bfloat16),
        in_specs=[vmem] * (5 + len(late)),
        out_specs=vmem,
        compiler_params=pltpu.CompilerParams(vmem_limit_bytes=OTHER_VMEM),
        name="pack",
    )(total, last_key, last_value, select, notes, *late)
    paired = packed.reshape(seq_count // 2, stride, 2, head_cols)
    sides = [list(range(side, seq_count, 2)) for side in range(2)]
    arrived = lax.all_to_all(
        paired, "seq", split_axis=0, concat_axis=0, tiled=True, axis_index_groups=sides
    ).reshape(packed.shape)
    shared = lax.ppermute(arrived, "seq", [(i, i ^ 1) for i in range(seq_count)])
    cache = jax.ShapeDtypeStruct((slot_total, draft, head_cols), jnp.bfloat16)
    half = [
        pltpu.VMEM((seq_count // 2, 2 * slot_cap * draft, head_cols), jnp.bfloat16),
        pltpu.VMEM((slot_cap, seq_count // 2 * draft, head_cols), jnp.float32),
    ]
    own = pl.pallas_call(
        functools.partial(place_own_kernel, slot_cap, draft, slot_total),
        out_shape=jax.ShapeDtypeStruct((slot_total * draft, 2 * head_cols), jnp.float32),
        in_specs=[smem, vmem],
        out_specs=vmem,
        scratch_shapes=half,
        cost_estimate=pl.CostEstimate(
            flops=4 * slot_total * draft * slot_total * draft * head_cols,
            bytes_accessed=4 * packed.size,
            transcendentals=0,
        ),
        compiler_params=pltpu.CompilerParams(vmem_limit_bytes=OTHER_VMEM),
        name="place_own",
    )(side, arrived)
    return pl.pallas_call(
        functools.partial(place_kernel, slot_cap),
        out_shape=(cache, cache),
        in_specs=[smem, vmem, vmem],
        out_specs=(vmem, vmem),
        scratch_shapes=half,
        compiler_params=pltpu.CompilerParams(vmem_limit_bytes=OTHER_VMEM),
        name="place",
    )(side, own, shared)


def solution(mesh):
    placed = (
        P(("grp", "seq"), "head"),
        P(None, "head"),
        P(None, "head"),
        P(("grp", "seq")),
        P(("grp", "seq")),
        P(("grp", "seq")),
    )
    return jax.shard_map(
        local,
        mesh=mesh,
        in_specs=placed,
        out_specs=(P(("grp", "seq"), None, "head"), P(("grp", "seq"), None, "head")),
        check_vma=False,
    )
```

```python
import functools

import jax
import jax.numpy as jnp
from jax import lax
from jax.experimental import pallas as pl
from jax.experimental.pallas import tpu as pltpu
from jax.sharding import PartitionSpec as P

CHUNKS = 2
PROJECT_VMEM = 99 * 2**19
OTHER_VMEM = 12 * 2**20


def gather_ring(block):
    heads, lines = lax.axis_size("head"), lax.axis_size("seq")

    def turn(step):
        return [
            (line * heads + i, line * heads + (i + (step if line % 2 == 0 else -step)) % heads)
            for line in range(lines)
            for i in range(heads)
        ]

    axes, up, down = ("seq", "head"), turn(1), turn(-1)
    own = jnp.split(block, CHUNKS, axis=0)
    held = [(0, own)]
    rising, falling = list(own), list(own)
    for step in range(1, (heads + 1) // 2):
        for c in range(CHUNKS):
            rising[c] = lax.ppermute(rising[c], axes, up)
            falling[c] = lax.ppermute(falling[c], axes, down)
        held.append((-step, list(rising)))
        held.append((step, list(falling)))
    if heads % 2 == 0:
        last = [
            lax.ppermute(rising[c], axes, up) if c % 2 == 0 else lax.ppermute(falling[c], axes, down)
            for c in range(CHUNKS)
        ]
        held.append((heads // 2, last))
    return held


def iota(shape, dim):
    return lax.broadcasted_iota(jnp.int32, shape, dim)


def project_kernel(offsets, slot_cap, draft, owners, me_ref, turn_ref, route_ref, wk_ref, wv_ref, *refs):
    count = len(offsets) - 1
    blocks = refs[: count * CHUNKS]
    total_ref, lastk_ref, lastv_ref, select_ref, notes_ref, weights, sems = refs[count * CHUNKS :]
    depth, head_cols = blocks[0].shape[1], wk_ref.shape[1]
    heads = len(offsets)
    fetches = []
    for i, offset in enumerate(offsets):
        origin = lax.rem(me_ref[0] + turn_ref[0] * offset + heads, heads)
        at = pl.ds(pl.multiple_of(origin * depth, depth), depth)
        to = (weights.at[i, 0], weights.at[i, 1]) if i < count else (lastk_ref, lastv_ref)
        for j, w in enumerate((wk_ref, wv_ref)):
            fetches.append(pltpu.make_async_copy(w.at[at, :], to[j], sems.at[2 * i + j]))
    for fetch in fetches:
        fetch.start()
    req = route_ref.shape[1]
    slots = owners * slot_cap
    route = route_ref[...]
    page = lax.rem(route, slots).astype(jnp.float32)
    owner = lax.rem(lax.div(route, slots), owners).astype(jnp.float32)
    accepted = lax.div(route, slots * owners).astype(jnp.float32)
    diagonal = iota((req, req), 0) == iota((req, req), 1)
    owner_col = jnp.sum(jnp.where(diagonal, owner, 0.0), axis=1, keepdims=True)
    earlier = (owner_col == owner) & (iota((req, req), 0) < iota((req, req), 1))
    within = jnp.sum(jnp.where(earlier, 1.0, 0.0), axis=0, keepdims=True)
    slot = owner * slot_cap + within
    row_count = req * draft
    lane, sub = iota((req, row_count), 1), iota((req, row_count), 0)
    mine = (lane >= sub * draft) & (lane < sub * draft + draft)
    slot_col = jnp.sum(jnp.where(diagonal, slot, 0.0), axis=1, keepdims=True)
    accepted_col = jnp.sum(jnp.where(diagonal, accepted, 0.0), axis=1, keepdims=True)
    draft_row = (lane - sub * draft).astype(jnp.float32)
    wanted = jnp.where(
        mine & (draft_row < accepted_col), slot_col * draft + draft_row + 1.0, 0.0
    )
    target = jnp.sum(wanted, axis=0, keepdims=True) - 1.0
    row = iota(select_ref.shape, 0).astype(jnp.float32)
    select_ref[...] = jnp.where(row == target, 1.0, 0.0).astype(jnp.bfloat16)
    taken = iota((notes_ref.shape[0], req), 0).astype(jnp.float32) == slot
    found = jnp.sum(jnp.where(taken, page + 1.0, 0.0), axis=1, keepdims=True)
    notes_ref[...] = jnp.broadcast_to(found, notes_ref.shape).astype(jnp.bfloat16)
    total = None
    for group in (range(count // 2), range(count // 2, count)):
        rows, both = [], []
        for i in group:
            fetches[2 * i].wait()
            fetches[2 * i + 1].wait()
            rows.append(
                jnp.concatenate([b[...] for b in blocks[i * CHUNKS : (i + 1) * CHUNKS]], axis=0)
            )
            both.append(jnp.concatenate([weights[i, 0], weights[i, 1]], axis=1))
        part = jnp.dot(
            jnp.concatenate(rows, axis=1),
            jnp.concatenate(both, axis=0),
            preferred_element_type=jnp.float32,
        )
        total = part if total is None else total + part
    total_ref[...] = total
    fetches[2 * count].wait()
    fetches[2 * count + 1].wait()


def pack_kernel(slot_cap, draft, total_ref, lastk_ref, lastv_ref, select_ref, notes_ref, *refs):
    out_ref = refs[-1]
    rows = jnp.concatenate([b[...] for b in refs[:-1]], axis=0)
    both = jnp.concatenate([lastk_ref[...], lastv_ref[...]], axis=1)
    total = total_ref[...] + jnp.dot(rows, both, preferred_element_type=jnp.float32)
    packed = jnp.dot(
        select_ref[...], total.astype(jnp.bfloat16), preferred_element_type=jnp.float32
    ).astype(jnp.bfloat16)
    head_cols = out_ref.shape[1]
    span = slot_cap * draft
    stride = 2 * span + slot_cap
    for d in range(out_ref.shape[0] // stride):
        at = d * stride
        out_ref[at : at + span, :] = packed[d * span : (d + 1) * span, :head_cols]
        out_ref[at + span : at + 2 * span, :] = packed[d * span : (d + 1) * span, head_cols:]
        out_ref[at + 2 * span : at + stride, :] = notes_ref[d * slot_cap : (d + 1) * slot_cap, :]


def place_part(slot_cap, draft, pages, side_ref, from_ref, rows_ref, notes_ref):
    head_cols = from_ref.shape[1]
    span = slot_cap * draft
    stride = 2 * span + slot_cap
    sources = rows_ref.shape[0]
    rows = sources * draft

    def take(side):
        for d in range(sources):
            at = (2 * d + side) * stride
            rows_ref[d] = from_ref[at : at + 2 * span, :]
            notes = from_ref[at + 2 * span : at + stride, :].astype(jnp.float32)
            for s in range(slot_cap):
                notes_ref[s, d * draft : (d + 1) * draft, :] = jnp.broadcast_to(
                    notes[s : s + 1, :], (draft, head_cols)
                )

    for side in range(2):
        pl.when(side_ref[0] == side)(functools.partial(take, side))
    draft_row = lax.rem(iota((rows, head_cols), 0), draft).astype(jnp.float32)
    total = None
    for s in range(slot_cap):
        page = notes_ref[s]
        goes = jnp.where(page > 0.0, (page - 1.0) * draft + draft_row, -1.0)
        select = jnp.concatenate(
            [
                jnp.where(goes == (iota(goes.shape, 1) + at).astype(jnp.float32), 1.0, 0.0)
                for at in range(0, pages * draft, head_cols)
            ],
            axis=1,
        ).astype(jnp.bfloat16)
        keys = rows_ref[:, s * draft : (s + 1) * draft, :].reshape(rows, head_cols)
        values = rows_ref[:, span + s * draft : span + (s + 1) * draft, :].reshape(rows, head_cols)
        both = jnp.concatenate([keys, values], axis=1)
        part = lax.dot_general(
            select, both, (((0,), (0,)), ((), ())), preferred_element_type=jnp.float32
        )
        total = part if total is None else total + part
    return total


def place_own_kernel(slot_cap, draft, pages, side_ref, own_ref, total_ref, rows_ref, notes_ref):
    total_ref[...] = place_part(slot_cap, draft, pages, side_ref, own_ref, rows_ref, notes_ref)


def place_kernel(slot_cap, side_ref, total_ref, other_ref, key_ref, value_ref, rows_ref, notes_ref):
    pages, draft, head_cols = key_ref.shape
    part = place_part(slot_cap, draft, pages, side_ref, other_ref, rows_ref, notes_ref)
    placed = (total_ref[...] + part).astype(jnp.bfloat16)
    key_ref[...] = placed[:, :head_cols].reshape(pages, draft, head_cols)
    value_ref[...] = placed[:, head_cols:].reshape(pages, draft, head_cols)


def local(draft_features, w_key, w_value, accepted, owner_group, page_slot):
    req_dev = accepted.shape[0]
    draft = draft_features.shape[0] // req_dev
    depth = draft_features.shape[1]
    head_cols = w_key.shape[1]
    seq_count = lax.axis_size("seq")
    slot_cap = max(2, 2 * req_dev // seq_count)
    slot_total = slot_cap * seq_count
    me = lax.axis_index("head").astype(jnp.int32).reshape(1)
    side = (lax.axis_index("seq") & 1).astype(jnp.int32).reshape(1)
    turn = 1 - 2 * side
    route = ((accepted * seq_count + owner_group) * slot_total + page_slot).reshape(1, req_dev)
    held = gather_ring(draft_features)
    offsets = tuple(offset for offset, _ in held)
    blocks = [b for _, chunks in held for b in chunks]
    vmem = pl.BlockSpec(memory_space=pltpu.VMEM)
    hbm = pl.BlockSpec(memory_space=pltpu.HBM)
    smem = pl.BlockSpec(memory_space=pltpu.SMEM)
    early, late = blocks[:-CHUNKS], blocks[-CHUNKS:]
    row_count, heads = req_dev * draft, len(offsets)
    stride = 2 * slot_cap * draft + slot_cap
    total, last_key, last_value, select, notes = pl.pallas_call(
        functools.partial(project_kernel, offsets, slot_cap, draft, seq_count),
        out_shape=(
            jax.ShapeDtypeStruct((row_count, 2 * head_cols), jnp.float32),
            jax.ShapeDtypeStruct((depth, head_cols), jnp.bfloat16),
            jax.ShapeDtypeStruct((depth, head_cols), jnp.bfloat16),
            jax.ShapeDtypeStruct((slot_total * draft, row_count), jnp.bfloat16),
            jax.ShapeDtypeStruct((slot_total, head_cols), jnp.bfloat16),
        ),
        in_specs=[smem, smem, vmem] + [hbm] * 2 + [vmem] * len(early),
        out_specs=(vmem,) * 5,
        scratch_shapes=[
            pltpu.VMEM((heads - 1, 2, depth, head_cols), jnp.bfloat16),
            pltpu.SemaphoreType.DMA((2 * heads,)),
        ],
        cost_estimate=pl.CostEstimate(
            flops=4 * row_count * depth * heads * head_cols,
            bytes_accessed=2 * (row_count + 2 * head_cols) * depth * heads,
            transcendentals=0,
        ),
        compiler_params=pltpu.CompilerParams(vmem_limit_bytes=PROJECT_VMEM),
        name="project",
    )(me, turn, route, w_key, w_value, *early)
    packed = pl.pallas_call(
        functools.partial(pack_kernel, slot_cap, draft),
        out_shape=jax.ShapeDtypeStruct((seq_count * stride, head_cols), jnp.bfloat16),
        in_specs=[vmem] * (5 + len(late)),
        out_specs=vmem,
        compiler_params=pltpu.CompilerParams(vmem_limit_bytes=OTHER_VMEM),
        name="pack",
    )(total, last_key, last_value, select, notes, *late)
    paired = packed.reshape(seq_count // 2, stride, 2, head_cols)
    sides = [list(range(side, seq_count, 2)) for side in range(2)]
    arrived = lax.all_to_all(
        paired, "seq", split_axis=0, concat_axis=0, tiled=True, axis_index_groups=sides
    ).reshape(packed.shape)
    shared = lax.ppermute(arrived, "seq", [(i, i ^ 1) for i in range(seq_count)])
    cache = jax.ShapeDtypeStruct((slot_total, draft, head_cols), jnp.bfloat16)
    half = [
        pltpu.VMEM((seq_count // 2, 2 * slot_cap * draft, head_cols), jnp.bfloat16),
        pltpu.VMEM((slot_cap, seq_count // 2 * draft, head_cols), jnp.float32),
    ]
    own = pl.pallas_call(
        functools.partial(place_own_kernel, slot_cap, draft, slot_total),
        out_shape=jax.ShapeDtypeStruct((slot_total * draft, 2 * head_cols), jnp.float32),
        in_specs=[smem, vmem],
        out_specs=vmem,
        scratch_shapes=half,
        cost_estimate=pl.CostEstimate(
            flops=4 * slot_total * draft * slot_total * draft * head_cols,
            bytes_accessed=4 * packed.size,
            transcendentals=0,
        ),
        compiler_params=pltpu.CompilerParams(vmem_limit_bytes=OTHER_VMEM),
        name="place_own",
    )(side, arrived)
    return pl.pallas_call(
        functools.partial(place_kernel, slot_cap),
        out_shape=(cache, cache),
        in_specs=[smem, vmem, vmem],
        out_specs=(vmem, vmem),
        scratch_shapes=half,
        compiler_params=pltpu.CompilerParams(vmem_limit_bytes=OTHER_VMEM),
        name="place",
    )(side, own, shared)


def solution(mesh):
    placed = (
        P(("grp", "seq"), "head"),
        P(None, "head"),
        P(None, "head"),
        P(("grp", "seq")),
        P(("grp", "seq")),
        P(("grp", "seq")),
    )
    return jax.shard_map(
        local,
        mesh=mesh,
        in_specs=placed,
        out_specs=(P(("grp", "seq"), None, "head"), P(("grp", "seq"), None, "head")),
        check_vma=False,
    )
```
